16 devices in a mesh: replica: 2 (over y, z), data: 8 (over x, core).
Axes of the slice: x: 4, y: 2, z: 1, core: 2. Of those that a mesh axis runs over, the one named last changes fastest.
The devices are a block of a 4x4x8 slice.
Arguments:
- x: bfloat16 [16384, 2048], P(('replica', 'data')), parts along dimension 0
- adapter_id: int32 [16384], P(('replica', 'data')), parts along dimension 0
- w_gate: bfloat16 [2048, 5632], replicated
- w_up: bfloat16 [2048, 5632], replicated
- w_down: bfloat16 [5632, 2048], replicated
- a_gate: bfloat16 [32, 2048, 64], P('data')
- b_gate: bfloat16 [32, 64, 5632], P('data')
- a_up: bfloat16 [32, 2048, 64], P('data')
- b_up: bfloat16 [32, 64, 5632], P('data')
- a_down: bfloat16 [32, 5632, 64], P('data')
- b_down: bfloat16 [32, 64, 2048], P('data')
- hot_ids: int32 [4], replicated
- hot_a_gate: bfloat16 [4, 2048, 64], replicated
- hot_b_gate: bfloat16 [4, 64, 5632], replicated
- hot_a_up: bfloat16 [4, 2048, 64], replicated
- hot_b_up: bfloat16 [4, 64, 5632], replicated
- hot_a_down: bfloat16 [4, 5632, 64], replicated
- hot_b_down: bfloat16 [4, 64, 2048], replicated
Outputs:
- output: bfloat16 [16384, 2048], P(('replica', 'data')), parts along dimension 0
There are 2 independent parts. The reference program is written for one: setup_inputs(seed, part) draws one part's arguments, and reference() takes and returns one part's arrays. A program takes and returns all parts, laid end to end along the dimension named above; an argument that names none is the same for every part.
All inputs are finite; a program needn't handle non-finite values.
Results may differ from the reference program's by a relative error of at most 0.00179.
Values are sent between devices in bfloat16 or wider.
A program may use at most 768 MiB of HBM per device.

```python
import jax
import jax.numpy as jnp
from jax import lax

GROUP = 8
T_LOC = 1024
D = 2048
F = 5632
R = 64
N_LOC = 4
HOT_K = 4
LORA_ALPHA = 32
TOK_BLOCK = 128
TOKENS = GROUP * T_LOC
ADAPTERS = GROUP * N_LOC
CAP = T_LOC // (2 * GROUP)
LORA_SCALE = LORA_ALPHA / R


def draw_hot(hot_key):
    owner_key, local_key = jax.random.split(hot_key)
    hot_owner = jax.random.permutation(owner_key, GROUP)[:HOT_K]
    hot_local = jax.random.randint(local_key, (HOT_K,), 0, N_LOC)
    return hot_owner, hot_local


def draw_ids(id_key, hot_owner, hot_local):
    shift_key, peak_key, count_key, perm_key, cold_key, pick_key = jax.random.split(id_key, 6)
    owners = jnp.arange(GROUP)
    peak_owner = jax.random.randint(peak_key, (), 0, GROUP)
    pop_shift = jnp.where(owners == peak_owner, 0, jax.random.randint(shift_key, (GROUP,), 0, 4))
    cap_upper = jnp.maximum(CAP // (2 ** pop_shift), 1)
    cap_lower = jnp.maximum(cap_upper // 2, 1)
    counts = jax.random.randint(count_key, (GROUP, GROUP), cap_lower[None, :], cap_upper[None, :] + 1)
    counts = jnp.where(owners[None, :] == peak_owner, CAP, counts)
    count_ends = jnp.cumsum(counts, axis=1)
    positions = jnp.arange(T_LOC)

    def owner_row(end_row):
        return jnp.searchsorted(end_row, positions, side='right')

    owner_seq = jax.vmap(owner_row)(count_ends)
    owner_seq = jax.random.permutation(perm_key, owner_seq, axis=1, independent=True)
    owner_safe = jnp.minimum(owner_seq, GROUP - 1)
    hot_match = hot_owner[None, :] == owners[:, None]
    has_hot = jnp.any(hot_match, axis=1).astype(jnp.int32)
    skip_local = jnp.sum(jnp.where(hot_match, hot_local[None, :], 0), axis=1) + (1 - has_hot) * N_LOC
    pick_local = jax.random.randint(cold_key, (GROUP, T_LOC), 0, N_LOC - has_hot[owner_safe])
    pick_local = pick_local + (pick_local >= skip_local[owner_safe]).astype(jnp.int32)
    cold_ids = owner_safe * N_LOC + pick_local
    hot_list = hot_owner * N_LOC + hot_local
    hot_tok = hot_list[jax.random.randint(pick_key, (GROUP, T_LOC), 0, HOT_K)]
    tok_ids = jnp.where(owner_seq == GROUP, hot_tok, cold_ids)
    return tok_ids.reshape(TOKENS).astype(jnp.int32)


def normal_weights(w_key, shape, std):
    return (jax.random.normal(w_key, shape, jnp.float32) * std).astype(jnp.bfloat16)


def adapter_set(set_key, adapter_count):
    set_keys = jax.random.split(set_key, 6)
    b_std = 0.5 / (LORA_SCALE * R ** 0.5)
    return [
        normal_weights(set_keys[0], (adapter_count, D, R), D ** -0.5),
        normal_weights(set_keys[1], (adapter_count, R, F), b_std),
        normal_weights(set_keys[2], (adapter_count, D, R), D ** -0.5),
        normal_weights(set_keys[3], (adapter_count, R, F), b_std),
        normal_weights(set_keys[4], (adapter_count, F, R), F ** -0.5),
        normal_weights(set_keys[5], (adapter_count, R, D), b_std),
    ]


def setup_inputs(seed: int = 0, part: int = 0) -> dict:
    root_key = jax.random.key(seed)
    base_keys = jax.random.split(jax.random.fold_in(root_key, 1), 3)
    route_key = jax.random.fold_in(root_key, 3)
    hot_owner, hot_local = draw_hot(jax.random.fold_in(route_key, 2))
    tok_ids = draw_ids(jax.random.fold_in(jax.random.fold_in(route_key, 1), part), hot_owner, hot_local)
    x_key = jax.random.fold_in(jax.random.fold_in(root_key, 5), part)
    store_set = adapter_set(jax.random.fold_in(root_key, 2), ADAPTERS)
    hot_set = adapter_set(jax.random.fold_in(root_key, 4), HOT_K)
    return {
        'x': jax.random.normal(x_key, (TOKENS, D), jnp.float32).astype(jnp.bfloat16),
        'adapter_id': tok_ids,
        'w_gate': normal_weights(base_keys[0], (D, F), D ** -0.5),
        'w_up': normal_weights(base_keys[1], (D, F), D ** -0.5),
        'w_down': normal_weights(base_keys[2], (F, D), F ** -0.5),
        'a_gate': store_set[0],
        'b_gate': store_set[1],
        'a_up': store_set[2],
        'b_up': store_set[3],
        'a_down': store_set[4],
        'b_down': store_set[5],
        'hot_ids': (hot_owner * N_LOC + hot_local).astype(jnp.int32),
        'hot_a_gate': hot_set[0],
        'hot_b_gate': hot_set[1],
        'hot_a_up': hot_set[2],
        'hot_b_up': hot_set[3],
        'hot_a_down': hot_set[4],
        'hot_b_down': hot_set[5],
    }


def lora_delta(tok_rows, a_rows, b_rows):
    low_rank = jnp.einsum('td,tdr->tr', tok_rows.astype(jnp.float32), a_rows.astype(jnp.float32)).astype(jnp.bfloat16)
    delta_f = jnp.einsum('tr,trf->tf', low_rank.astype(jnp.float32), b_rows.astype(jnp.float32))
    return (LORA_SCALE * delta_f).astype(jnp.bfloat16)


def reference(x, adapter_id, w_gate, w_up, w_down, a_gate, b_gate, a_up, b_up, a_down, b_down, hot_ids, hot_a_gate, hot_b_gate, hot_a_up, hot_b_up, hot_a_down, hot_b_down):
    def block_out(block_args):
        tok_rows, tok_ids = block_args
        hot_match = tok_ids[:, None] == hot_ids[None, :]
        is_hot = jnp.any(hot_match, axis=1)
        hot_slot = jnp.sum(jnp.where(hot_match, jnp.arange(HOT_K)[None, :], 0), axis=1)

        def chosen(store_set, hot_copy):
            return jnp.where(is_hot[:, None, None], hot_copy[hot_slot], store_set[tok_ids])

        gate_act = jnp.dot(tok_rows, w_gate, preferred_element_type=jnp.float32) + lora_delta(tok_rows, chosen(a_gate, hot_a_gate), chosen(b_gate, hot_b_gate)).astype(jnp.float32)
        up_act = jnp.dot(tok_rows, w_up, preferred_element_type=jnp.float32) + lora_delta(tok_rows, chosen(a_up, hot_a_up), chosen(b_up, hot_b_up)).astype(jnp.float32)
        hidden = (jax.nn.silu(gate_act) * up_act).astype(jnp.bfloat16)
        down_out = jnp.dot(hidden, w_down, preferred_element_type=jnp.float32) + lora_delta(hidden, chosen(a_down, hot_a_down), chosen(b_down, hot_b_down)).astype(jnp.float32)
        return (tok_rows.astype(jnp.float32) + down_out).astype(jnp.bfloat16)

    blocks = lax.map(block_out, (x.reshape(TOKENS // TOK_BLOCK, TOK_BLOCK, D), adapter_id.reshape(TOKENS // TOK_BLOCK, TOK_BLOCK)))
    return blocks.reshape(TOKENS, D)
```

```python
import functools

import jax
import jax.numpy as jnp
from jax import lax
from jax.experimental import pallas as pl
from jax.experimental.pallas import tpu as pltpu
from jax.sharding import PartitionSpec as P

LORA_ALPHA = 32
BF16, F32, I32 = jnp.bfloat16, jnp.float32, jnp.int32
MESH = pl.DeviceIdType.MESH
GU_COLS = 512
SUB_COLS = 256
DN_COLS = 256


def nt_dot(rows, mat):
    return lax.dot_general(rows, mat, (((1,), (1,)), ((), ())), preferred_element_type=F32)


def nn_dot(rows, mat):
    return jnp.dot(rows, mat, preferred_element_type=F32)


def route(ids, hot_ids_ref, group, n_local, n_hot, cap):
    tok = ids.shape[1]
    hot = jnp.zeros(ids.shape, jnp.bool_)
    slot = jnp.zeros(ids.shape, I32)
    for j in range(n_hot):
        match = ids == hot_ids_ref[j]
        hot = hot | match
        slot = jnp.where(match, j, slot)
    owner = lax.div(ids, jnp.full(ids.shape, n_local, I32))
    slot = jnp.where(hot, slot, n_hot + ids - owner * n_local)
    key = jnp.where(hot, group, owner)
    n_rows = -(-(group + 1) // 16) * 16
    marks = (lax.broadcasted_iota(I32, (n_rows, tok), 0) == key).astype(F32)
    lane = 128
    before = (lax.broadcasted_iota(I32, (lane, lane), 0) < lax.broadcasted_iota(I32, (lane, lane), 1)).astype(F32).astype(BF16)
    total = jnp.zeros((n_rows, 1), F32)
    ranks = []
    for b in range(tok // lane):
        part = marks[:, b * lane:(b + 1) * lane]
        ranks.append(nn_dot(part.astype(BF16), before) + total)
        total = total + jnp.sum(part, axis=1, keepdims=True)
    rank = jnp.concatenate(ranks, axis=1)
    hot_rank = rank[group:group + 1, :]
    spare = jnp.zeros((1, 1), F32)
    place = jnp.zeros(ids.shape, F32)
    placed = jnp.zeros(ids.shape, F32)
    for j in range(group):
        count = total[j:j + 1, :]
        room = cap - count
        cold_place = rank[j:j + 1, :] + float(j * cap)
        place = jnp.where(key == j, cold_place, place)
        fits = (key == group) & (hot_rank >= spare) & (hot_rank < spare + room)
        place = jnp.where(fits, hot_rank - spare + (count + float(j * cap)), place)
        placed = jnp.where(fits, 1.0, placed)
        spare = spare + room
    kept = (key == group) & (placed == 0.0)
    place = jnp.where(kept, hot_rank - spare + float(group * cap), place)
    return place, slot.astype(F32)


def main_kernel(cfg, ids_ref, hot_ref, x_ref, wg_ref, wu_ref, wd_ref, ag_ref, bg_ref, au_ref, bu_ref, ad_ref, bd_ref,
                hag_ref, hbg_ref, hau_ref, hbu_ref, had_ref, hbd_ref,
                place_ref, back_ref, kept_ref,
                xs, meta, recv, recv_meta, h_kept, h_recv, at_g, at_u, at_d, b_d, wg, wu, bg, bu, wd, low_g, low_u, low_d,
                x_sem, w_sem, d_sem, a_sem, out_sem, send_sem, got_sem, msend_sem, mgot_sem, bsend_sem, bgot_sem):
    group, cap, n_local, n_hot, rank_dim, scale = cfg
    tok, dim = x_ref.shape
    hidden = wg_ref.shape[1]
    half = tok // 2
    hot_w, store_w = n_hot * rank_dim, n_local * rank_dim
    gu_tiles, dn_tiles = hidden // GU_COLS, dim // DN_COLS
    me = lax.axis_index("data")

    barrier = pltpu.get_barrier_semaphore()
    for k in range(1, group):
        pl.semaphore_signal(barrier, inc=1, device_id={"data": lax.rem(me + k, group)}, device_id_type=MESH)

    x_copies = [pltpu.make_async_copy(x_ref.at[pl.ds(i * half, half), :], h_recv.at[:, pl.ds(i * dim, dim)], x_sem.at[i]) for i in range(2)]
    for c in x_copies:
        c.start()
    adapters = [
        pltpu.make_async_copy(hag_ref, at_g.at[pl.ds(0, hot_w), :], a_sem.at[0]),
        pltpu.make_async_copy(hau_ref, at_u.at[pl.ds(0, hot_w), :], a_sem.at[1]),
        pltpu.make_async_copy(ag_ref, at_g.at[pl.ds(hot_w, store_w), :], a_sem.at[2]),
        pltpu.make_async_copy(au_ref, at_u.at[pl.ds(hot_w, store_w), :], a_sem.at[3]),
        pltpu.make_async_copy(had_ref, at_d.at[pl.ds(0, hot_w), :], a_sem.at[4]),
        pltpu.make_async_copy(ad_ref, at_d.at[pl.ds(hot_w, store_w), :], a_sem.at[5]),
        pltpu.make_async_copy(hbd_ref, b_d.at[pl.ds(0, hot_w), :], a_sem.at[6]),
        pltpu.make_async_copy(bd_ref, b_d.at[pl.ds(hot_w, store_w), :], a_sem.at[7]),
    ]

    def gu_copies(step):
        cols = pl.ds(pl.multiple_of(lax.rem(step, gu_tiles) * GU_COLS, GU_COLS), GU_COLS)
        s = lax.rem(step, 2)
        return [
            pltpu.make_async_copy(wg_ref.at[:, cols], wg.at[s], w_sem.at[s, 0]),
            pltpu.make_async_copy(wu_ref.at[:, cols], wu.at[s], w_sem.at[s, 1]),
            pltpu.make_async_copy(hbg_ref.at[:, cols], bg.at[s, pl.ds(0, hot_w), :], w_sem.at[s, 2]),
            pltpu.make_async_copy(hbu_ref.at[:, cols], bu.at[s, pl.ds(0, hot_w), :], w_sem.at[s, 3]),
            pltpu.make_async_copy(bg_ref.at[:, cols], bg.at[s, pl.ds(hot_w, store_w), :], w_sem.at[s, 4]),
            pltpu.make_async_copy(bu_ref.at[:, cols], bu.at[s, pl.ds(hot_w, store_w), :], w_sem.at[s, 5]),
        ]

    def dn_copy(step):
        cols = pl.ds(pl.multiple_of(lax.rem(step, dn_tiles) * DN_COLS, DN_COLS), DN_COLS)
        s = lax.rem(step, 2)
        return pltpu.make_async_copy(wd_ref.at[:, cols], wd.at[s], d_sem.at[s])

    for c in adapters[:2]:
        c.start()
    for c in gu_copies(jnp.int32(0)):
        c.start()
    for c in adapters[2:]:
        c.start()
    dn_copy(jnp.int32(0)).start()

    place, slot = route(ids_ref[...], hot_ref, group, n_local, n_hot, float(cap))
    place_i = place.astype(I32)
    slot_b = jnp.broadcast_to(slot, (128, tok)).astype(BF16)
    for c in x_copies:
        c.wait()

    def sort_rows(first, count):
        sel = (lax.broadcasted_iota(I32, (count, tok), 0) + first == place_i).astype(F32).astype(BF16)
        meta[pl.ds(first, count), :] = nt_dot(sel, slot_b).astype(BF16)
        for n in range(0, dim, 512):
            rows = nn_dot(sel[:, :half], h_recv[:, n:n + 512]) + nn_dot(sel[:, half:], h_recv[:, dim + n:dim + n + 512])
            xs[pl.ds(first, count), n:n + 512] = rows.astype(BF16)

    sort_rows(0, 256)
    sort_rows(256, 256)

    pl.semaphore_wait(barrier, group - 1)

    def x_copy(k):
        peer = lax.rem(me + k, group)
        src, dst = pl.ds(pl.multiple_of(peer * cap, cap), cap), pl.ds(pl.multiple_of(me * cap, cap), cap)
        return (
            pltpu.make_async_remote_copy(xs.at[src, :], recv.at[dst, :], send_sem.at[k - 1], got_sem.at[k - 1], device_id={"data": peer}, device_id_type=MESH),
            pltpu.make_async_remote_copy(meta.at[src, :], recv_meta.at[dst, :], msend_sem.at[k - 1], mgot_sem.at[k - 1], device_id={"data": peer}, device_id_type=MESH),
        )

    for k in range(1, group):
        for c in x_copy(k):
            c.start()

    sort_rows(512, 256)
    sort_rows(768, 256)
    place_ref[...] = jnp.transpose(jnp.broadcast_to(place, (128, tok))).astype(I32)
    mine = pl.ds(pl.multiple_of(me * cap, cap), cap)
    recv[mine, :] = xs[mine, :]
    recv_meta[mine, :] = meta[mine, :]

    def keep(low, slots, width):
        cols = jnp.concatenate([slots.astype(F32)] * (width // 128), axis=1)
        lanes = lax.div(lax.broadcasted_iota(I32, cols.shape, 1), jnp.full(cols.shape, rank_dim, I32)).astype(F32)
        return jnp.where(cols == lanes, low, 0.0).astype(BF16)

    def delta(low, mat):
        return (scale * nn_dot(low, mat)).astype(BF16).astype(F32)

    def gate_up(rows_ref, rows, slots, width, h_ref, first_step):
        low_g[:, :width] = keep(nt_dot(rows_ref[rows, :], at_g[:width, :]), slots, width)
        low_u[:, :width] = keep(nt_dot(rows_ref[rows, :], at_u[:width, :]), slots, width)

        @pl.loop(0, gu_tiles)
        def _(i):
            step = i + first_step
            for c in gu_copies(step):
                c.wait()

            @pl.when(step + 1 < 2 * gu_tiles)
            def _():
                for c in gu_copies(step + 1):
                    c.start()

            s = lax.rem(step, 2)
            for n in range(0, GU_COLS, SUB_COLS):
                sub = slice(n, n + SUB_COLS)
                g = nn_dot(rows_ref[rows, :], wg[s, :, sub]) + delta(low_g[:, :width], bg[s, :width, sub])
                u = nn_dot(rows_ref[rows, :], wu[s, :, sub]) + delta(low_u[:, :width], bu[s, :width, sub])
                h_ref[:, pl.ds(pl.multiple_of(i * GU_COLS + n, SUB_COLS), SUB_COLS)] = (jax.nn.silu(g) * u).astype(BF16)

    for c in adapters[:2]:
        c.wait()
    kept_rows = slice(half, tok)
    gate_up(xs, kept_rows, meta[kept_rows, :], hot_w, h_kept, 0)

    for c in adapters[2:]:
        c.wait()
    for k in range(1, group):
        for c in x_copy(k):
            c.wait_recv()
    gate_up(recv, slice(0, half), recv_meta[...], hot_w + store_w, h_recv, gu_tiles)

    def back_copy(p, k):
        peer = lax.rem(me + k, group)
        cols = pl.ds(pl.multiple_of(p * (2 * DN_COLS), 2 * DN_COLS), 2 * DN_COLS)
        return pltpu.make_async_remote_copy(
            recv.at[pl.ds(pl.multiple_of(peer * cap, cap), cap), cols], back_ref.at[pl.ds(pl.multiple_of(me * cap, cap), cap), cols],
            bsend_sem.at[p, k - 1], bgot_sem.at[p, k - 1], device_id={"data": peer}, device_id_type=MESH)

    def down(h_ref, rows_ref, rows, slots, width, first_step, after):
        low_d[:, :width] = keep(nt_dot(h_ref[...], at_d[:width, :]), slots, width)

        @pl.loop(0, dn_tiles // 2)
        def _(p):
            for q in range(2):
                i = p * 2 + q
                step = i + first_step
                dn_copy(step).wait()

                @pl.when(step + 1 < 2 * dn_tiles)
                def _():
                    dn_copy(step + 1).start()

                cols = pl.ds(pl.multiple_of(i * DN_COLS, DN_COLS), DN_COLS)
                y = nn_dot(h_ref[...], wd[lax.rem(step, 2)]) + delta(low_d[:, :width], b_d[:width, cols])
                rows_ref[rows, cols] = (rows_ref[rows, cols].astype(F32) + y).astype(BF16)
            after(p)

    def send_back(p):
        for k in range(1, group):
            back_copy(p, k).start()

    down(h_recv, recv, slice(0, half), recv_meta[...], hot_w + store_w, 0, send_back)
    own = pltpu.make_async_copy(recv.at[mine, :], back_ref.at[mine, :], out_sem.at[0])
    own.start()
    down(h_kept, xs, kept_rows, meta[kept_rows, :], hot_w, dn_tiles, lambda p: None)
    kept_out = pltpu.make_async_copy(xs.at[pl.ds(half, half), :], kept_ref, out_sem.at[1])
    kept_out.start()
    own.wait()
    kept_out.wait()
    for k in range(1, group):
        for c in x_copy(k):
            c.wait_send()

    @pl.loop(0, dn_tiles // 2)
    def _(p):
        for k in range(1, group):
            back_copy(p, k).wait()


def unsort_kernel(place_ref, back_ref, kept_ref, out_ref):
    count, half = out_ref.shape[0], back_ref.shape[0]
    dim = out_ref.shape[1]
    place = jnp.concatenate([place_ref[...]] * (2 * half // 128), axis=1)
    sel = (place == lax.broadcasted_iota(I32, (count, 2 * half), 1)).astype(F32).astype(BF16)
    for n in range(0, dim, 512):
        rows = nn_dot(sel[:, :half], back_ref[:, n:n + 512]) + nn_dot(sel[:, half:], kept_ref[:, n:n + 512])
        out_ref[:, n:n + 512] = rows.astype(BF16)


def solution(mesh):
    group = mesh.shape["data"]
    token_spec = P(("replica", "data"), None)
    store_spec = P("data", None, None)
    full_mat = P(None, None)
    full_set = P(None, None, None)
    in_specs = (token_spec, P(("replica", "data")), full_mat, full_mat, full_mat) + (store_spec,) * 6 + (P(None),) + (full_set,) * 6

    def device_step(x, adapter_id, w_gate, w_up, w_down, a_gate, b_gate, a_up, b_up, a_down, b_down, hot_ids, hot_a_gate, hot_b_gate, hot_a_up, hot_b_up, hot_a_down, hot_b_down):
        tok, dim = x.shape
        hidden = w_gate.shape[1]
        n_local, _, rank_dim = a_gate.shape
        n_hot = hot_ids.shape[0]
        cap = tok // (2 * group)
        half = tok // 2
        both = (n_hot + n_local) * rank_dim
        cfg = (group, cap, n_local, n_hot, rank_dim, LORA_ALPHA / rank_dim)

        def rows_of(a):
            return jnp.swapaxes(a, 1, 2).reshape(-1, a.shape[1])

        def flat(b):
            return b.reshape(-1, b.shape[2])

        any_spec = pl.BlockSpec(memory_space=pl.ANY)
        vmem_spec = pl.BlockSpec(memory_space=pltpu.VMEM)
        dma = pltpu.SemaphoreType.DMA
        place, back, kept = pl.pallas_call(
            functools.partial(main_kernel, cfg),
            out_shape=(
                jax.ShapeDtypeStruct((tok, 128), I32),
                jax.ShapeDtypeStruct((half, dim), BF16),
                jax.ShapeDtypeStruct((half, dim), BF16),
            ),
            in_specs=[vmem_spec, pl.BlockSpec(memory_space=pltpu.SMEM)] + [any_spec] * 16,
            out_specs=(vmem_spec, any_spec, any_spec),
            scratch_shapes=[
                pltpu.VMEM((tok, dim), BF16),
                pltpu.VMEM((tok, 128), BF16),
                pltpu.VMEM((half, dim), BF16),
                pltpu.VMEM((half, 128), BF16),
                pltpu.VMEM((half, hidden), BF16),
                pltpu.VMEM((half, hidden), BF16),
                pltpu.VMEM((both, dim), BF16),
                pltpu.VMEM((both, dim), BF16),
                pltpu.VMEM((both, hidden), BF16),
                pltpu.VMEM((both, dim), BF16),
                pltpu.VMEM((2, dim, GU_COLS), BF16),
                pltpu.VMEM((2, dim, GU_COLS), BF16),
                pltpu.VMEM((2, both, GU_COLS), BF16),
                pltpu.VMEM((2, both, GU_COLS), BF16),
                pltpu.VMEM((2, hidden, DN_COLS), BF16),
                pltpu.VMEM((half, both), BF16),
                pltpu.VMEM((half, both), BF16),
                pltpu.VMEM((half, both), BF16),
                dma((2,)), dma((2, 6)), dma((2,)), dma((8,)), dma((2,)),
                dma((group - 1,)), dma((group - 1,)), dma((group - 1,)), dma((group - 1,)),
                dma((dim // DN_COLS // 2, group - 1)), dma((dim // DN_COLS // 2, group - 1)),
            ],
            compiler_params=pltpu.CompilerParams(collective_id=0, has_side_effects=True, vmem_limit_bytes=66_000_000),
            name="mlp_exchange",
        )(adapter_id.reshape(1, tok), hot_ids, x, w_gate, w_up, w_down,
          rows_of(a_gate), flat(b_gate), rows_of(a_up), flat(b_up), rows_of(a_down), flat(b_down),
          rows_of(hot_a_gate), flat(hot_b_gate), rows_of(hot_a_up), flat(hot_b_up), rows_of(hot_a_down), flat(hot_b_down))

        block = 256
        return pl.pallas_call(
            unsort_kernel,
            grid=(tok // block,),
            out_shape=jax.ShapeDtypeStruct((tok, dim), BF16),
            in_specs=[
                pl.BlockSpec((block, 128), lambda i: (i, 0)),
                pl.BlockSpec((half, dim), lambda i: (0, 0)),
                pl.BlockSpec((half, dim), lambda i: (0, 0)),
            ],
            out_specs=pl.BlockSpec((block, dim), lambda i: (i, 0)),
            name="unsort",
        )(place, back, kept)

    return jax.shard_map(device_step, mesh=mesh, in_specs=in_specs, out_specs=token_spec, check_vma=False)
```

```python
import functools

import jax
import jax.numpy as jnp
from jax import lax
from jax.experimental import pallas as pl
from jax.experimental.pallas import tpu as pltpu
from jax.sharding import PartitionSpec as P

LORA_ALPHA = 32
BF16, F32, I32 = jnp.bfloat16, jnp.float32, jnp.int32
MESH = pl.DeviceIdType.MESH
GU_COLS = 512
SUB_ROWS = 256
DN_COLS = 512
LOAD_COLS = 512


def nt_dot(rows, mat):
    return lax.dot_general(rows, mat, (((1,), (1,)), ((), ())), preferred_element_type=F32)


def nn_dot(rows, mat):
    return jnp.dot(rows, mat, preferred_element_type=F32)


def route(ids, hot_ids_ref, group, n_local, n_hot, cap):
    tok = ids.shape[1]
    hot = jnp.zeros(ids.shape, jnp.bool_)
    slot = jnp.zeros(ids.shape, I32)
    for j in range(n_hot):
        match = ids == hot_ids_ref[j]
        hot = hot | match
        slot = jnp.where(match, j, slot)
    owner = lax.div(ids, jnp.full(ids.shape, n_local, I32))
    slot = jnp.where(hot, slot, n_hot + ids - owner * n_local)
    key = jnp.where(hot, group, owner)
    rows = -(-(group + 1) // 16) * 16
    lane = 128
    blocks = tok // lane
    marks = (lax.broadcasted_iota(I32, (rows, tok), 0) == key).astype(F32)
    stacked = jnp.concatenate([marks[:, b * lane:(b + 1) * lane] for b in range(blocks)], axis=0).astype(BF16)
    r, c = lax.broadcasted_iota(I32, (lane, 2 * lane), 0), lax.broadcasted_iota(I32, (lane, 2 * lane), 1)
    counted = nn_dot(stacked, ((r < c) | (c >= lane)).astype(F32).astype(BF16))
    total = jnp.zeros((rows, lane), F32)
    ranks = []
    for b in range(blocks):
        part = counted[b * rows:(b + 1) * rows, :]
        ranks.append(part[:, :lane] + total)
        total = total + part[:, lane:]
    row = lax.broadcasted_iota(I32, (rows, lane), 0)
    room = jnp.where(row < group, cap - total, 0.0)
    before = jnp.zeros((rows, lane), F32)
    for j in range(group):
        before = before + jnp.where(row > j, room[j:j + 1, :], 0.0)
    base = row.astype(F32) * cap
    all_room = before[group:group + 1, :]
    places = []
    for b in range(blocks):
        mark, rank = marks[:, b * lane:(b + 1) * lane], ranks[b]
        is_hot, hot_rank = mark[group:group + 1, :] > 0.0, rank[group:group + 1, :]
        fits = is_hot & (row < group) & (hot_rank >= before) & (hot_rank < before + room)
        spots = jnp.where(fits, hot_rank - before + total + base, 0.0)
        spots = jnp.where((mark > 0.0) & (row < group), rank + base, spots)
        place = jnp.sum(spots, axis=0, keepdims=True)
        places.append(jnp.where(is_hot & (hot_rank >= all_room), hot_rank - all_room + group * cap, place))
    return jnp.concatenate(places, axis=1), slot.astype(F32)


def main_kernel(cfg, ids_ref, hot_ref, x_ref, wg_ref, wu_ref, wd_ref, ag_ref, bg_ref, au_ref, bu_ref, ad_ref, bd_ref,
                hag_ref, hbg_ref, hau_ref, hbu_ref, had_ref, hbd_ref,
                place_ref, back_ref, kept_ref,
                xs, meta, recv, recv_meta, h_kept, h_recv, at_g, at_u, at_d, b_d, wg, wu, bg, bu, wd, low_g, low_u, low_d, place_t,
                x_sem, w_sem, d_sem, a_sem, out_sem, send_sem, got_sem, msend_sem, mgot_sem, bsend_sem, bgot_sem, kept_sem):
    group, cap, n_local, n_hot, rank_dim, scale = cfg
    tok, dim = x_ref.shape
    hidden = wg_ref.shape[1]
    half = tok // 2
    hot_w, store_w = n_hot * rank_dim, n_local * rank_dim
    gu_tiles, dn_tiles = hidden // GU_COLS, dim // DN_COLS
    me = lax.axis_index("data")

    barrier = pltpu.get_barrier_semaphore()
    for k in range(1, group):
        pl.semaphore_signal(barrier, inc=1, device_id={"data": lax.rem(me + k, group)}, device_id_type=MESH)

    x_copies = [pltpu.make_async_copy(x_ref.at[pl.ds(i * half, half), :], h_recv.at[:, pl.ds(i * dim, dim)], x_sem.at[i]) for i in range(2)]
    for c in x_copies:
        c.start(priority=0)
    adapters = [
        pltpu.make_async_copy(hag_ref, at_g.at[pl.ds(0, hot_w), :], a_sem.at[0]),
        pltpu.make_async_copy(hau_ref, at_u.at[pl.ds(0, hot_w), :], a_sem.at[1]),
        pltpu.make_async_copy(ag_ref, at_g.at[pl.ds(hot_w, store_w), :], a_sem.at[2]),
        pltpu.make_async_copy(au_ref, at_u.at[pl.ds(hot_w, store_w), :], a_sem.at[3]),
        pltpu.make_async_copy(had_ref, at_d.at[pl.ds(0, hot_w), :], a_sem.at[4]),
        pltpu.make_async_copy(ad_ref, at_d.at[pl.ds(hot_w, store_w), :], a_sem.at[5]),
        pltpu.make_async_copy(hbd_ref, b_d.at[pl.ds(0, hot_w), :], a_sem.at[6]),
        pltpu.make_async_copy(bd_ref, b_d.at[pl.ds(hot_w, store_w), :], a_sem.at[7]),
    ]

    def gu_place(step):
        return pl.ds(pl.multiple_of(lax.rem(step, gu_tiles) * GU_COLS, GU_COLS), GU_COLS), lax.rem(step, 2)

    def store_b_copies(step):
        cols, s = gu_place(step)
        return [
            pltpu.make_async_copy(bg_ref.at[:, cols], bg.at[s, pl.ds(hot_w, store_w), :], w_sem.at[s, 4]),
            pltpu.make_async_copy(bu_ref.at[:, cols], bu.at[s, pl.ds(hot_w, store_w), :], w_sem.at[s, 5]),
        ]

    def gu_copies(step, with_store):
        cols, s = gu_place(step)
        return [
            pltpu.make_async_copy(wg_ref.at[:, cols], wg.at[s], w_sem.at[s, 0]),
            pltpu.make_async_copy(wu_ref.at[:, cols], wu.at[s], w_sem.at[s, 1]),
            pltpu.make_async_copy(hbg_ref.at[:, cols], bg.at[s, pl.ds(0, hot_w), :], w_sem.at[s, 2]),
            pltpu.make_async_copy(hbu_ref.at[:, cols], bu.at[s, pl.ds(0, hot_w), :], w_sem.at[s, 3]),
        ] + (store_b_copies(step) if with_store else [])

    def dn_copy(step):
        cols = pl.ds(pl.multiple_of(lax.rem(step, dn_tiles) * DN_COLS, DN_COLS), DN_COLS)
        s = lax.rem(step, 2)
        part = hidden // 2
        return [pltpu.make_async_copy(wd_ref.at[pl.ds(j * part, part), cols], wd.at[s, pl.ds(j * part, part), :], d_sem.at[s, j]) for j in range(2)]

    for c in adapters[:2] + gu_copies(jnp.int32(0), False):
        c.start(priority=1)

    place, slot = route(ids_ref[...], hot_ref, group, n_local, n_hot, float(cap))
    place_i = place.astype(I32)
    slot_b = jnp.broadcast_to(slot, (128, tok)).astype(BF16)
    for c in x_copies:
        c.wait()

    def sort_rows(first, count):
        sel = (lax.broadcasted_iota(I32, (count, tok), 0) + first == place_i).astype(F32).astype(BF16)
        meta[pl.ds(first, count), :] = nt_dot(sel, slot_b).astype(BF16)
        for n in range(0, dim, 512):
            rows = nn_dot(sel[:, :half], h_recv[:, n:n + 512]) + nn_dot(sel[:, half:], h_recv[:, dim + n:dim + n + 512])
            xs[pl.ds(first, count), n:n + 512] = rows.astype(BF16)

    sort_rows(0, 256)
    sort_rows(256, 256)

    pl.semaphore_wait(barrier, group - 1)

    def x_copy(k):
        peer = lax.rem(me + k, group)
        src, dst = pl.ds(pl.multiple_of(peer * cap, cap), cap), pl.ds(pl.multiple_of(me * cap, cap), cap)
        return (
            pltpu.make_async_remote_copy(xs.at[src, :], recv.at[dst, :], send_sem.at[k - 1], got_sem.at[k - 1], device_id={"data": peer}, device_id_type=MESH),
            pltpu.make_async_remote_copy(meta.at[src, :], recv_meta.at[dst, :], msend_sem.at[k - 1], mgot_sem.at[k - 1], device_id={"data": peer}, device_id_type=MESH),
        )

    for k in range(1, group):
        for c in x_copy(k):
            c.start()

    for c in adapters[2:] + dn_copy(jnp.int32(0)):
        c.start(priority=1)

    sort_rows(512, 256)
    sort_rows(768, 256)
    place_t[...] = jnp.transpose(jnp.broadcast_to(place, (128, tok))).astype(I32)
    place_out = pltpu.make_async_copy(place_t, place_ref, out_sem.at[1])
    place_out.start()
    mine = pl.ds(pl.multiple_of(me * cap, cap), cap)
    recv[mine, :] = xs[mine, :]
    recv_meta[mine, :] = meta[mine, :]

    def keep(low, slots, width):
        cols = jnp.concatenate([slots.astype(F32)] * (width // 128), axis=1)
        lanes = lax.div(lax.broadcasted_iota(I32, cols.shape, 1), jnp.full(cols.shape, rank_dim, I32)).astype(F32)
        return jnp.where(cols == lanes, low, 0.0).astype(BF16)

    def delta(low, mat):
        return (scale * nn_dot(low, mat)).astype(BF16).astype(F32)

    def gate_up(rows_ref, rows, slots, width, h_ref, first_step):
        low_g[:, :width] = keep(nt_dot(rows_ref[rows, :], at_g[:width, :]), slots, width)
        low_u[:, :width] = keep(nt_dot(rows_ref[rows, :], at_u[:width, :]), slots, width)

        @pl.loop(0, gu_tiles)
        def _(i):
            step = i + first_step
            for c in gu_copies(step, width > hot_w):
                c.wait()

            @pl.when(step + 1 < 2 * gu_tiles)
            def _():
                for j, c in enumerate(gu_copies(step + 1, False)):
                    c.start(priority=j % 2)

            @pl.when((step + 1 >= gu_tiles) & (step + 1 < 2 * gu_tiles))
            def _():
                for j, c in enumerate(store_b_copies(step + 1)):
                    c.start(priority=j % 2)

            s = lax.rem(step, 2)
            cols = pl.ds(pl.multiple_of(i * GU_COLS, GU_COLS), GU_COLS)
            for m in range(0, half, SUB_ROWS):
                sub, src = slice(m, m + SUB_ROWS), slice(rows.start + m, rows.start + m + SUB_ROWS)
                g = nn_dot(rows_ref[src, :], wg[s]) + delta(low_g[sub, :width], bg[s, :width, :])
                u = nn_dot(rows_ref[src, :], wu[s]) + delta(low_u[sub, :width], bu[s, :width, :])
                h_ref[sub, cols] = (jax.nn.silu(g) * u).astype(BF16)

    for c in adapters[:2]:
        c.wait()
    kept_rows = slice(half, tok)
    gate_up(xs, kept_rows, meta[kept_rows, :], hot_w, h_kept, 0)

    for c in adapters[2:]:
        c.wait()
    for k in range(1, group):
        for c in x_copy(k):
            c.wait_recv()
    gate_up(recv, slice(0, half), recv_meta[...], hot_w + store_w, h_recv, gu_tiles)

    def back_copy(p, k):
        peer = lax.rem(me + k, group)
        cols = pl.ds(pl.multiple_of(p * (DN_COLS), DN_COLS), DN_COLS)
        return pltpu.make_async_remote_copy(
            recv.at[pl.ds(pl.multiple_of(peer * cap, cap), cap), cols], back_ref.at[pl.ds(pl.multiple_of(me * cap, cap), cap), cols],
            bsend_sem.at[p, k - 1], bgot_sem.at[p, k - 1], device_id={"data": peer}, device_id_type=MESH)

    def down(h_ref, rows_ref, rows, slots, width, first_step, after):
        low_d[:, :width] = keep(nt_dot(h_ref[...], at_d[:width, :]), slots, width)

        @pl.loop(0, dn_tiles)
        def _(p):
            step = p + first_step
            for c in dn_copy(step):
                c.wait()

            @pl.when(step + 1 < 2 * dn_tiles)
            def _():
                for j, c in enumerate(dn_copy(step + 1)):
                    c.start(priority=j)

            cols = pl.ds(pl.multiple_of(p * DN_COLS, DN_COLS), DN_COLS)
            for m in range(0, half, SUB_ROWS):
                sub, src = slice(m, m + SUB_ROWS), slice(rows.start + m, rows.start + m + SUB_ROWS)
                y = nn_dot(h_ref[sub, :], wd[lax.rem(step, 2)]) + delta(low_d[sub, :width], b_d[:width, cols])
                rows_ref[src, cols] = (rows_ref[src, cols].astype(F32) + y).astype(BF16)
            after(p)

    def send_back(p):
        for k in range(1, group):
            back_copy(p, k).start()

    down(h_recv, recv, slice(0, half), recv_meta[...], hot_w + store_w, 0, send_back)
    own = pltpu.make_async_copy(recv.at[mine, :], back_ref.at[mine, :], out_sem.at[0])
    own.start()

    def kept_copy(p):
        cols = pl.ds(pl.multiple_of(p * DN_COLS, DN_COLS), DN_COLS)
        return pltpu.make_async_copy(xs.at[pl.ds(half, half), cols], kept_ref.at[:, cols], kept_sem.at[p])

    down(h_kept, xs, kept_rows, meta[kept_rows, :], hot_w, dn_tiles, lambda p: kept_copy(p).start())
    own.wait()
    place_out.wait()
    for k in range(1, group):
        for c in x_copy(k):
            c.wait_send()

    @pl.loop(0, dn_tiles)
    def _(p):
        for k in range(1, group):
            back_copy(p, k).wait()
        kept_copy(p).wait()


def unsort_kernel(place_ref, back_ref, kept_ref, out_ref, place, rows, sel, done, sem, out_sem):
    tok, dim = out_ref.shape
    half = tok // 2

    def load(n):
        cols = pl.ds(n * LOAD_COLS, LOAD_COLS)
        return [pltpu.make_async_copy(ref.at[:, cols], rows.at[pl.ds(j * half, half), cols], sem.at[n, j]) for j, ref in enumerate((back_ref, kept_ref))]

    n_stores = (tok // 256) * (dim // LOAD_COLS)

    def store(i):
        n, t = divmod(i, tok // 256)
        return pltpu.make_async_copy(done.at[i % 4], out_ref.at[pl.ds(t * 256, 256), pl.ds(n * LOAD_COLS, LOAD_COLS)], out_sem.at[i % 4])

    first = pltpu.make_async_copy(place_ref, place, sem.at[dim // LOAD_COLS, 0])
    first.start(priority=0)
    for n in range(dim // LOAD_COLS):
        for c in load(n):
            c.start(priority=1)
    first.wait()
    for t in range(0, tok, 256):
        spots = jnp.concatenate([place[t:t + 256, :]] * (tok // 128), axis=1)
        sel[t:t + 256, :] = (spots == lax.broadcasted_iota(I32, (256, tok), 1)).astype(F32).astype(BF16)
    for n in range(dim // LOAD_COLS):
        for c in load(n):
            c.wait()
        cols = slice(n * LOAD_COLS, (n + 1) * LOAD_COLS)
        for t in range(0, tok, 256):
            i = n * (tok // 256) + t // 256
            if i >= 4:
                store(i - 4).wait()
            done[i % 4] = (nn_dot(sel[t:t + 256, :half], rows[:half, cols]) + nn_dot(sel[t:t + 256, half:], rows[half:, cols])).astype(BF16)
            store(i).start()
    for i in range(n_stores - 4, n_stores):
        store(i).wait()


def solution(mesh):
    group = mesh.shape["data"]
    token_spec = P(("replica", "data"), None)
    store_spec = P("data", None, None)
    full_mat = P(None, None)
    full_set = P(None, None, None)
    in_specs = (token_spec, P(("replica", "data")), full_mat, full_mat, full_mat) + (store_spec,) * 6 + (P(None),) + (full_set,) * 6

    def device_step(x, adapter_id, w_gate, w_up, w_down, a_gate, b_gate, a_up, b_up, a_down, b_down, hot_ids, hot_a_gate, hot_b_gate, hot_a_up, hot_b_up, hot_a_down, hot_b_down):
        tok, dim = x.shape
        hidden = w_gate.shape[1]
        n_local, _, rank_dim = a_gate.shape
        n_hot = hot_ids.shape[0]
        cap = tok // (2 * group)
        half = tok // 2
        both = (n_hot + n_local) * rank_dim
        cfg = (group, cap, n_local, n_hot, rank_dim, LORA_ALPHA / rank_dim)

        def rows_of(a):
            return jnp.swapaxes(a, 1, 2).reshape(-1, a.shape[1])

        def flat(b):
            return b.reshape(-1, b.shape[2])

        any_spec = pl.BlockSpec(memory_space=pl.ANY)
        vmem_spec = pl.BlockSpec(memory_space=pltpu.VMEM)
        dma = pltpu.SemaphoreType.DMA
        place, back, kept = pl.pallas_call(
            functools.partial(main_kernel, cfg),
            out_shape=(
                jax.ShapeDtypeStruct((tok, 128), I32),
                jax.ShapeDtypeStruct((half, dim), BF16),
                jax.ShapeDtypeStruct((half, dim), BF16),
            ),
            in_specs=[vmem_spec, pl.BlockSpec(memory_space=pltpu.SMEM)] + [any_spec] * 16,
            out_specs=(any_spec, any_spec, any_spec),
            scratch_shapes=[
                pltpu.VMEM((tok, dim), BF16),
                pltpu.VMEM((tok, 128), BF16),
                pltpu.VMEM((half, dim), BF16),
                pltpu.VMEM((half, 128), BF16),
                pltpu.VMEM((half, hidden), BF16),
                pltpu.VMEM((half, hidden), BF16),
                pltpu.VMEM((both, dim), BF16),
                pltpu.VMEM((both, dim), BF16),
                pltpu.VMEM((both, hidden), BF16),
                pltpu.VMEM((both, dim), BF16),
                pltpu.VMEM((2, dim, GU_COLS), BF16),
                pltpu.VMEM((2, dim, GU_COLS), BF16),
                pltpu.VMEM((2, both, GU_COLS), BF16),
                pltpu.VMEM((2, both, GU_COLS), BF16),
                pltpu.VMEM((2, hidden, DN_COLS), BF16),
                pltpu.VMEM((half, both), BF16),
                pltpu.VMEM((half, both), BF16),
                pltpu.VMEM((half, both), BF16),
                pltpu.VMEM((tok, 128), I32),
                dma((2,)), dma((2, 6)), dma((2, 2)), dma((8,)), dma((2,)),
                dma((group - 1,)), dma((group - 1,)), dma((group - 1,)), dma((group - 1,)),
                dma((dim // DN_COLS, group - 1)), dma((dim // DN_COLS, group - 1)), dma((dim // DN_COLS,)),
            ],
            compiler_params=pltpu.CompilerParams(collective_id=0, has_side_effects=True, vmem_limit_bytes=66_000_000),
            name="mlp_exchange",
        )(adapter_id.reshape(1, tok), hot_ids, x, w_gate, w_up, w_down,
          rows_of(a_gate), flat(b_gate), rows_of(a_up), flat(b_up), rows_of(a_down), flat(b_down),
          rows_of(hot_a_gate), flat(hot_b_gate), rows_of(hot_a_up), flat(hot_b_up), rows_of(hot_a_down), flat(hot_b_down))

        return pl.pallas_call(
            unsort_kernel,
            out_shape=jax.ShapeDtypeStruct((tok, dim), BF16),
            in_specs=[any_spec] * 3,
            out_specs=any_spec,
            scratch_shapes=[
                pltpu.VMEM((tok, 128), I32),
                pltpu.VMEM((tok, dim), BF16),
                pltpu.VMEM((tok, tok), BF16),
                pltpu.VMEM((4, 256, LOAD_COLS), BF16),
                dma((dim // LOAD_COLS + 1, 2)),
                dma((4,)),
            ],
            name="unsort",
        )(place, back, kept)

    return jax.shard_map(device_step, mesh=mesh, in_specs=in_specs, out_specs=token_spec, check_vma=False)
```

```python
import functools

import jax
import jax.numpy as jnp
from jax import lax
from jax.experimental import pallas as pl
from jax.experimental.pallas import tpu as pltpu
from jax.sharding import PartitionSpec as P

LORA_ALPHA = 32
BF16, F32, I32 = jnp.bfloat16, jnp.float32, jnp.int32
MESH = pl.DeviceIdType.MESH
BLOCK = 512
SUB_ROWS = 256
UNSORT_COLS = 256


def nt_dot(rows, mat):
    return lax.dot_general(rows, mat, (((1,), (1,)), ((), ())), preferred_element_type=F32)


def nn_dot(rows, mat):
    return jnp.dot(rows, mat, preferred_element_type=F32)


def route(ids, hot_ids_ref, group, n_local, n_hot, cap):
    tok = ids.shape[1]
    hot = jnp.zeros(ids.shape, jnp.bool_)
    slot = jnp.zeros(ids.shape, I32)
    for j in range(n_hot):
        match = ids == hot_ids_ref[j]
        hot = hot | match
        slot = jnp.where(match, j, slot)
    owner = lax.div(ids, jnp.full(ids.shape, n_local, I32))
    slot = jnp.where(hot, slot, n_hot + ids - owner * n_local)
    key = jnp.where(hot, group, owner)
    rows = -(-(group + 1) // 16) * 16
    lane = 128
    blocks = tok // lane
    marks = (lax.broadcasted_iota(I32, (rows, tok), 0) == key).astype(F32)
    stacked = jnp.concatenate([marks[:, b * lane:(b + 1) * lane] for b in range(blocks)], axis=0).astype(BF16)
    r, c = lax.broadcasted_iota(I32, (lane, 2 * lane), 0), lax.broadcasted_iota(I32, (lane, 2 * lane), 1)
    counted = nn_dot(stacked, ((r < c) | (c >= lane)).astype(F32).astype(BF16))
    total = jnp.zeros((rows, lane), F32)
    ranks = []
    for b in range(blocks):
        part = counted[b * rows:(b + 1) * rows, :]
        ranks.append(part[:, :lane] + total)
        total = total + part[:, lane:]
    row = lax.broadcasted_iota(I32, (rows, lane), 0)
    room = jnp.where(row < group, cap - total, 0.0)
    before = jnp.zeros((rows, lane), F32)
    for j in range(group):
        before = before + jnp.where(row > j, room[j:j + 1, :], 0.0)
    base = row.astype(F32) * cap
    all_room = before[group:group + 1, :]
    places = []
    for b in range(blocks):
        mark, rank = marks[:, b * lane:(b + 1) * lane], ranks[b]
        is_hot, hot_rank = mark[group:group + 1, :] > 0.0, rank[group:group + 1, :]
        fits = is_hot & (row < group) & (hot_rank >= before) & (hot_rank < before + room)
        spots = jnp.where(fits, hot_rank - before + total + base, 0.0)
        spots = jnp.where((mark > 0.0) & (row < group), rank + base, spots)
        place = jnp.sum(spots, axis=0, keepdims=True)
        places.append(jnp.where(is_hot & (hot_rank >= all_room), hot_rank - all_room + group * cap, place))
    return jnp.concatenate(places, axis=1), slot.astype(F32)


def main_kernel(cfg, ids_ref, hot_ref, x_ref, wg_ref, wu_ref, wd_ref, ag_ref, bg_ref, au_ref, bu_ref, ad_ref, bd_ref,
                hag_ref, hbg_ref, hau_ref, hbu_ref, had_ref, hbd_ref,
                place_ref, back_ref, kept_ref,
                xs, meta, recv, recv_meta, h_kept, h_recv, at_g, at_u, at_d, b_d, arena, low_g, low_u, low_d, place_t,
                x_sem, w_sem, d_sem, a_sem, out_sem, send_sem, got_sem, msend_sem, mgot_sem, bsend_sem, bgot_sem, kept_sem):
    group, cap, n_local, n_hot, rank_dim, scale = cfg
    tok, dim = x_ref.shape
    hidden = wg_ref.shape[1]
    half = tok // 2
    hot_w, store_w = n_hot * rank_dim, n_local * rank_dim
    gu_tiles, dn_tiles = hidden // BLOCK, dim // BLOCK
    gu_pairs, both = gu_tiles // 2, hot_w + store_w
    me = lax.axis_index("data")

    barrier = pltpu.get_barrier_semaphore()
    for k in range(1, group):
        pl.semaphore_signal(barrier, inc=1, device_id={"data": lax.rem(me + k, group)}, device_id_type=MESH)

    x_copies = [pltpu.make_async_copy(x_ref.at[pl.ds(i * half, half), pl.ds(n, BLOCK)], h_recv.at[:, pl.ds(i * dim + n, BLOCK)], x_sem.at[n // BLOCK, i])
                for n in range(0, dim, BLOCK) for i in range(2)]
    for c in x_copies:
        c.start(priority=0)
    adapters = [
        pltpu.make_async_copy(hag_ref, at_g.at[pl.ds(0, hot_w), :], a_sem.at[0]),
        pltpu.make_async_copy(hau_ref, at_u.at[pl.ds(0, hot_w), :], a_sem.at[1]),
        pltpu.make_async_copy(ag_ref, at_g.at[pl.ds(hot_w, store_w), :], a_sem.at[2]),
        pltpu.make_async_copy(au_ref, at_u.at[pl.ds(hot_w, store_w), :], a_sem.at[3]),
        pltpu.make_async_copy(had_ref, at_d.at[pl.ds(0, hot_w), :], a_sem.at[4]),
        pltpu.make_async_copy(ad_ref, at_d.at[pl.ds(hot_w, store_w), :], a_sem.at[5]),
        pltpu.make_async_copy(hbd_ref, b_d.at[pl.ds(0, hot_w), :], a_sem.at[6]),
        pltpu.make_async_copy(bd_ref, b_d.at[pl.ds(hot_w, store_w), :], a_sem.at[7]),
    ]

    g_row, u_row = 0, 2 * dim
    bg_row, bu_row = 4 * dim, 4 * dim + 2 * both

    def gu_copies(pair, s, with_store):
        copies = []
        for q in range(2):
            cols = pl.ds(pl.multiple_of(lax.rem(2 * pair + q, gu_tiles) * BLOCK, BLOCK), BLOCK)
            parts = [(wg_ref, g_row + q * dim, dim), (wu_ref, u_row + q * dim, dim),
                     (hbg_ref, bg_row + q * both, hot_w), (hbu_ref, bu_row + q * both, hot_w)]
            if with_store:
                parts += [(bg_ref, bg_row + q * both + hot_w, store_w), (bu_ref, bu_row + q * both + hot_w, store_w)]
            for j, (ref, first, count) in enumerate(parts):
                copies.append(pltpu.make_async_copy(ref.at[:, cols], arena.at[s, pl.ds(first, count), :], w_sem.at[s, q, j]))
        return copies

    def dn_copies(pair, s):
        copies = []
        for q in range(2):
            cols = pl.ds(pl.multiple_of(lax.rem(2 * pair + q, dn_tiles) * BLOCK, BLOCK), BLOCK)
            copies.append(pltpu.make_async_copy(wd_ref.at[:, cols], arena.at[s, pl.ds(q * hidden, hidden), :], d_sem.at[s, q]))
        return copies

    def start(copies):
        for j, c in enumerate(copies):
            c.start(priority=j % 2)

    def wait(copies):
        for c in copies:
            c.wait()

    for c in adapters[:2] + gu_copies(0, 0, False):
        c.start(priority=1)

    place, slot = route(ids_ref[...], hot_ref, group, n_local, n_hot, float(cap))
    place_i = place.astype(I32)
    slot_b = jnp.broadcast_to(slot, (128, tok)).astype(BF16)
    def sort_rows(first, arrive):
        sels = []
        for m in range(first, first + half, SUB_ROWS):
            sel = (lax.broadcasted_iota(I32, (SUB_ROWS, tok), 0) + m == place_i).astype(F32).astype(BF16)
            meta[pl.ds(m, SUB_ROWS), :] = nt_dot(sel, slot_b).astype(BF16)
            sels.append(sel)
        for n in range(0, dim, BLOCK):
            if arrive:
                for i in range(2):
                    x_copies[n // BLOCK * 2 + i].wait()
            for j, sel in enumerate(sels):
                rows = nn_dot(sel[:, :half], h_recv[:, n:n + BLOCK]) + nn_dot(sel[:, half:], h_recv[:, dim + n:dim + n + BLOCK])
                xs[pl.ds(first + j * SUB_ROWS, SUB_ROWS), n:n + BLOCK] = rows.astype(BF16)

    sort_rows(0, True)

    pl.semaphore_wait(barrier, group - 1)

    def x_copy(k):
        peer = lax.rem(me + k, group)
        src, dst = pl.ds(pl.multiple_of(peer * cap, cap), cap), pl.ds(pl.multiple_of(me * cap, cap), cap)
        return (
            pltpu.make_async_remote_copy(xs.at[src, :], recv.at[dst, :], send_sem.at[k - 1], got_sem.at[k - 1], device_id={"data": peer}, device_id_type=MESH),
            pltpu.make_async_remote_copy(meta.at[src, :], recv_meta.at[dst, :], msend_sem.at[k - 1], mgot_sem.at[k - 1], device_id={"data": peer}, device_id_type=MESH),
        )

    for k in range(1, group):
        for c in x_copy(k):
            c.start()

    for c in adapters[2:]:
        c.start(priority=1)

    sort_rows(half, False)
    place_t[...] = jnp.transpose(jnp.broadcast_to(place, (128, tok))).astype(I32)
    place_out = pltpu.make_async_copy(place_t, place_ref, out_sem.at[1])
    place_out.start()
    mine = pl.ds(pl.multiple_of(me * cap, cap), cap)
    recv[mine, :] = xs[mine, :]
    recv_meta[mine, :] = meta[mine, :]

    def keep(low, slots, width):
        cols = jnp.concatenate([slots.astype(F32)] * (width // 128), axis=1)
        lanes = lax.div(lax.broadcasted_iota(I32, cols.shape, 1), jnp.full(cols.shape, rank_dim, I32)).astype(F32)
        return jnp.where(cols == lanes, low, 0.0).astype(BF16)

    def delta(low, mat):
        return (scale * nn_dot(low, mat)).astype(BF16).astype(F32)

    def gate_up(rows_ref, rows, slots, width, h_ref, start_next):
        low_g[:, :width] = keep(nt_dot(rows_ref[rows, :], at_g[:width, :]), slots, width)
        low_u[:, :width] = keep(nt_dot(rows_ref[rows, :], at_u[:width, :]), slots, width)
        with_store = width > hot_w

        def block(tile, s, q):
            cols = pl.ds(pl.multiple_of(tile * BLOCK, BLOCK), BLOCK)
            for m in range(0, half, SUB_ROWS):
                sub, src = slice(m, m + SUB_ROWS), slice(rows.start + m, rows.start + m + SUB_ROWS)
                g = nn_dot(rows_ref[src, :], arena[s, g_row + q * dim:g_row + (q + 1) * dim, :])
                g = g + delta(low_g[sub, :width], arena[s, bg_row + q * both:bg_row + q * both + width, :])
                u = nn_dot(rows_ref[src, :], arena[s, u_row + q * dim:u_row + (q + 1) * dim, :])
                u = u + delta(low_u[sub, :width], arena[s, bu_row + q * both:bu_row + q * both + width, :])
                h_ref[sub, cols] = (jax.nn.silu(g) * u).astype(BF16)

        @pl.loop(0, gu_pairs)
        def _(i):
            s = lax.rem(i, 2)
            wait(gu_copies(i, s, with_store))
            start(gu_copies(i + 1, 1 - s, with_store))
            for q in range(2):
                block(2 * i + q, s, q)

        s = gu_pairs % 2
        wait(gu_copies(gu_pairs, s, with_store))
        start_next()
        block(gu_tiles - 1, s, 0)

    for c in adapters[:2]:
        c.wait()
    kept_rows = slice(half, tok)
    gate_up(xs, kept_rows, meta[kept_rows, :], hot_w, h_kept, lambda: start(gu_copies(0, 0, True)))

    for c in adapters[2:]:
        c.wait()
    for k in range(1, group):
        for c in x_copy(k):
            c.wait_recv()
    gate_up(recv, slice(0, half), recv_meta[...], both, h_recv, lambda: start(dn_copies(0, 0)))

    def back_copy(p, k):
        peer = lax.rem(me + k, group)
        cols = pl.ds(pl.multiple_of(p * (BLOCK), BLOCK), BLOCK)
        return pltpu.make_async_remote_copy(
            recv.at[pl.ds(pl.multiple_of(peer * cap, cap), cap), cols], back_ref.at[pl.ds(pl.multiple_of(me * cap, cap), cap), cols],
            bsend_sem.at[p, k - 1], bgot_sem.at[p, k - 1], device_id={"data": peer}, device_id_type=MESH)

    def down(h_ref, rows_ref, rows, slots, width, after):
        low_d[:, :width] = keep(nt_dot(h_ref[...], at_d[:width, :]), slots, width)

        @pl.loop(0, dn_tiles // 2)
        def _(i):
            s = lax.rem(i, 2)
            wait(dn_copies(i, s))
            start(dn_copies(i + 1, 1 - s))
            for q in range(2):
                p = 2 * i + q
                cols = pl.ds(pl.multiple_of(p * BLOCK, BLOCK), BLOCK)
                for m in range(0, half, SUB_ROWS):
                    sub, src = slice(m, m + SUB_ROWS), slice(rows.start + m, rows.start + m + SUB_ROWS)
                    y = nn_dot(h_ref[sub, :], arena[s, q * hidden:(q + 1) * hidden, :]) + delta(low_d[sub, :width], b_d[:width, cols])
                    rows_ref[src, cols] = (rows_ref[src, cols].astype(F32) + y).astype(BF16)
                after(p)

    def send_back(p):
        for k in range(1, group):
            back_copy(p, k).start()

    down(h_recv, recv, slice(0, half), recv_meta[...], both, send_back)
    own = pltpu.make_async_copy(recv.at[mine, :], back_ref.at[mine, :], out_sem.at[0])
    own.start()

    def kept_copy(p):
        cols = pl.ds(pl.multiple_of(p * BLOCK, BLOCK), BLOCK)
        return pltpu.make_async_copy(xs.at[pl.ds(half, half), cols], kept_ref.at[:, cols], kept_sem.at[p])

    down(h_kept, xs, kept_rows, meta[kept_rows, :], hot_w, lambda p: kept_copy(p).start())
    wait(dn_copies(0, 0))
    own.wait()
    place_out.wait()
    for k in range(1, group):
        for c in x_copy(k):
            c.wait_send()

    @pl.loop(0, dn_tiles)
    def _(p):
        for k in range(1, group):
            back_copy(p, k).wait()
        kept_copy(p).wait()


def unsort_kernel(place_ref, back_ref, kept_ref, out_ref, sel):
    tok, half = out_ref.shape[0], back_ref.shape[0]

    @pl.when(pl.program_id(0) == 0)
    def _():
        place = jnp.concatenate([place_ref[...]] * (tok // 128), axis=1)
        sel[...] = (place == lax.broadcasted_iota(I32, (tok, tok), 1)).astype(F32).astype(BF16)

    for n in range(0, out_ref.shape[1], UNSORT_COLS):
        cols = slice(n, n + UNSORT_COLS)
        rows = nn_dot(sel[:, :half], back_ref[:, cols]) + nn_dot(sel[:, half:], kept_ref[:, cols])
        out_ref[:, cols] = rows.astype(BF16)


def solution(mesh):
    group = mesh.shape["data"]
    token_spec = P(("replica", "data"), None)
    store_spec = P("data", None, None)
    full_mat = P(None, None)
    full_set = P(None, None, None)
    in_specs = (token_spec, P(("replica", "data")), full_mat, full_mat, full_mat) + (store_spec,) * 6 + (P(None),) + (full_set,) * 6

    def device_step(x, adapter_id, w_gate, w_up, w_down, a_gate, b_gate, a_up, b_up, a_down, b_down, hot_ids, hot_a_gate, hot_b_gate, hot_a_up, hot_b_up, hot_a_down, hot_b_down):
        tok, dim = x.shape
        hidden = w_gate.shape[1]
        n_local, _, rank_dim = a_gate.shape
        n_hot = hot_ids.shape[0]
        cap = tok // (2 * group)
        half = tok // 2
        both = (n_hot + n_local) * rank_dim
        cfg = (group, cap, n_local, n_hot, rank_dim, LORA_ALPHA / rank_dim)

        def rows_of(a):
            return jnp.swapaxes(a, 1, 2).reshape(-1, a.shape[1])

        def flat(b):
            return b.reshape(-1, b.shape[2])

        any_spec = pl.BlockSpec(memory_space=pl.ANY)
        vmem_spec = pl.BlockSpec(memory_space=pltpu.VMEM)
        dma = pltpu.SemaphoreType.DMA
        place, back, kept = pl.pallas_call(
            functools.partial(main_kernel, cfg),
            out_shape=(
                jax.ShapeDtypeStruct((tok, 128), I32),
                jax.ShapeDtypeStruct((half, dim), BF16),
                jax.ShapeDtypeStruct((half, dim), BF16),
            ),
            in_specs=[vmem_spec, pl.BlockSpec(memory_space=pltpu.SMEM)] + [any_spec] * 16,
            out_specs=(any_spec, any_spec, any_spec),
            scratch_shapes=[
                pltpu.VMEM((tok, dim), BF16),
                pltpu.VMEM((tok, 128), BF16),
                pltpu.VMEM((half, dim), BF16),
                pltpu.VMEM((half, 128), BF16),
                pltpu.VMEM((half, hidden), BF16),
                pltpu.VMEM((half, hidden), BF16),
                pltpu.VMEM((both, dim), BF16),
                pltpu.VMEM((both, dim), BF16),
                pltpu.VMEM((both, hidden), BF16),
                pltpu.VMEM((both, dim), BF16),
                pltpu.VMEM((2, max(4 * dim + 4 * both, 2 * hidden), BLOCK), BF16),
                pltpu.VMEM((half, both), BF16),
                pltpu.VMEM((half, both), BF16),
                pltpu.VMEM((half, both), BF16),
                pltpu.VMEM((tok, 128), I32),
                dma((dim // BLOCK, 2)), dma((2, 2, 6)), dma((2, 2)), dma((8,)), dma((2,)),
                dma((group - 1,)), dma((group - 1,)), dma((group - 1,)), dma((group - 1,)),
                dma((dim // BLOCK, group - 1)), dma((dim // BLOCK, group - 1)), dma((dim // BLOCK,)),
            ],
            compiler_params=pltpu.CompilerParams(collective_id=0, has_side_effects=True, vmem_limit_bytes=66_000_000),
            name="mlp_exchange",
        )(adapter_id.reshape(1, tok), hot_ids, x, w_gate, w_up, w_down,
          rows_of(a_gate), flat(b_gate), rows_of(a_up), flat(b_up), rows_of(a_down), flat(b_down),
          rows_of(hot_a_gate), flat(hot_b_gate), rows_of(hot_a_up), flat(hot_b_up), rows_of(hot_a_down), flat(hot_b_down))

        block = 512
        return pl.pallas_call(
            unsort_kernel,
            grid=(dim // block,),
            out_shape=jax.ShapeDtypeStruct((tok, dim), BF16),
            in_specs=[
                pl.BlockSpec((tok, 128), lambda i: (0, 0)),
                pl.BlockSpec((half, block), lambda i: (0, i)),
                pl.BlockSpec((half, block), lambda i: (0, i)),
            ],
            out_specs=pl.BlockSpec((tok, block), lambda i: (0, i)),
            scratch_shapes=[pltpu.VMEM((tok, tok), BF16)],
            name="unsort",
        )(place, back, kept)

    return jax.shard_map(device_step, mesh=mesh, in_specs=in_specs, out_specs=token_spec, check_vma=False)
```

```python
import functools

import jax
import jax.numpy as jnp
from jax import lax
from jax.experimental import pallas as pl
from jax.experimental.pallas import tpu as pltpu
from jax.sharding import PartitionSpec as P

LORA_ALPHA = 32
BF16, F32, I32 = jnp.bfloat16, jnp.float32, jnp.int32
MESH = pl.DeviceIdType.MESH
BLOCK = 512
SUB_ROWS = 256


def nt_dot(rows, mat):
    return lax.dot_general(rows, mat, (((1,), (1,)), ((), ())), preferred_element_type=F32)


def nn_dot(rows, mat):
    return jnp.dot(rows, mat, preferred_element_type=F32)


def route(ids, hot_ids_ref, group, n_local, n_hot, cap):
    tok = ids.shape[1]
    hot = jnp.zeros(ids.shape, jnp.bool_)
    slot = jnp.zeros(ids.shape, I32)
    for j in range(n_hot):
        match = ids == hot_ids_ref[j]
        hot = hot | match
        slot = jnp.where(match, j, slot)
    owner = lax.div(ids, jnp.full(ids.shape, n_local, I32))
    slot = jnp.where(hot, slot, n_hot + ids - owner * n_local)
    key = jnp.where(hot, group, owner)
    rows = -(-(group + 1) // 16) * 16
    lane = 128
    blocks = tok // lane
    marks = (lax.broadcasted_iota(I32, (rows, tok), 0) == key).astype(F32)
    stacked = jnp.concatenate([marks[:, b * lane:(b + 1) * lane] for b in range(blocks)], axis=0).astype(BF16)
    r, c = lax.broadcasted_iota(I32, (lane, 2 * lane), 0), lax.broadcasted_iota(I32, (lane, 2 * lane), 1)
    counted = nn_dot(stacked, ((r < c) | (c >= lane)).astype(F32).astype(BF16))
    total = jnp.zeros((rows, lane), F32)
    ranks = []
    for b in range(blocks):
        part = counted[b * rows:(b + 1) * rows, :]
        ranks.append(part[:, :lane] + total)
        total = total + part[:, lane:]
    row = lax.broadcasted_iota(I32, (rows, lane), 0)
    room = jnp.where(row < group, cap - total, 0.0)
    before = jnp.zeros((rows, lane), F32)
    for j in range(group):
        before = before + jnp.where(row > j, room[j:j + 1, :], 0.0)
    base = row.astype(F32) * cap
    all_room = before[group:group + 1, :]
    places = []
    for b in range(blocks):
        mark, rank = marks[:, b * lane:(b + 1) * lane], ranks[b]
        is_hot, hot_rank = mark[group:group + 1, :] > 0.0, rank[group:group + 1, :]
        fits = is_hot & (row < group) & (hot_rank >= before) & (hot_rank < before + room)
        spots = jnp.where(fits, hot_rank - before + total + base, 0.0)
        spots = jnp.where((mark > 0.0) & (row < group), rank + base, spots)
        place = jnp.sum(spots, axis=0, keepdims=True)
        places.append(jnp.where(is_hot & (hot_rank >= all_room), hot_rank - all_room + group * cap, place))
    return jnp.concatenate(places, axis=1), slot.astype(F32)


def main_kernel(cfg, ids_ref, hot_ref, x_ref, wg_ref, wu_ref, wd_ref, ag_ref, bg_ref, au_ref, bu_ref, ad_ref, bd_ref,
                hag_ref, hbg_ref, hau_ref, hbu_ref, had_ref, hbd_ref,
                place_ref, back_ref, kept_ref,
                xs, meta, recv, recv_meta, h_kept, h_recv, at_g, at_u, at_d, b_d, arena, low_g, low_u, low_d, place_t,
                x_sem, w_sem, d_sem, a_sem, out_sem, send_sem, got_sem, msend_sem, mgot_sem, bsend_sem, bgot_sem, kept_sem):
    group, cap, n_local, n_hot, rank_dim, scale = cfg
    tok, dim = x_ref.shape
    hidden = wg_ref.shape[1]
    half = tok // 2
    hot_w, store_w = n_hot * rank_dim, n_local * rank_dim
    gu_tiles, dn_tiles = hidden // BLOCK, dim // BLOCK
    gu_pairs, both = gu_tiles // 2, hot_w + store_w
    me = lax.axis_index("data")

    barrier = pltpu.get_barrier_semaphore()
    for k in range(1, group):
        pl.semaphore_signal(barrier, inc=1, device_id={"data": lax.rem(me + k, group)}, device_id_type=MESH)

    x_copies = [pltpu.make_async_copy(x_ref.at[pl.ds(i * half, half), pl.ds(n, BLOCK)], h_recv.at[:, pl.ds(i * dim + n, BLOCK)], x_sem.at[n // BLOCK, i])
                for n in range(0, dim, BLOCK) for i in range(2)]
    for c in x_copies:
        c.start(priority=0)
    adapters = [
        pltpu.make_async_copy(hag_ref, at_g.at[pl.ds(0, hot_w), :], a_sem.at[0]),
        pltpu.make_async_copy(hau_ref, at_u.at[pl.ds(0, hot_w), :], a_sem.at[1]),
        pltpu.make_async_copy(ag_ref, at_g.at[pl.ds(hot_w, store_w), :], a_sem.at[2]),
        pltpu.make_async_copy(au_ref, at_u.at[pl.ds(hot_w, store_w), :], a_sem.at[3]),
        pltpu.make_async_copy(had_ref, at_d.at[pl.ds(0, hot_w), :], a_sem.at[4]),
        pltpu.make_async_copy(ad_ref, at_d.at[pl.ds(hot_w, store_w), :], a_sem.at[5]),
        pltpu.make_async_copy(hbd_ref, b_d.at[pl.ds(0, hot_w), :], a_sem.at[6]),
        pltpu.make_async_copy(bd_ref, b_d.at[pl.ds(hot_w, store_w), :], a_sem.at[7]),
    ]

    g_row, u_row = 0, 2 * dim
    bg_row, bu_row = 4 * dim, 4 * dim + 2 * both

    def gu_copies(pair, s, with_store):
        copies = []
        for q in range(2):
            cols = pl.ds(pl.multiple_of(lax.rem(2 * pair + q, gu_tiles) * BLOCK, BLOCK), BLOCK)
            parts = [(wg_ref, g_row + q * dim, dim), (wu_ref, u_row + q * dim, dim),
                     (hbg_ref, bg_row + q * both, hot_w), (hbu_ref, bu_row + q * both, hot_w)]
            if with_store:
                parts += [(bg_ref, bg_row + q * both + hot_w, store_w), (bu_ref, bu_row + q * both + hot_w, store_w)]
            for j, (ref, first, count) in enumerate(parts):
                copies.append(pltpu.make_async_copy(ref.at[:, cols], arena.at[s, pl.ds(first, count), :], w_sem.at[s, q, j]))
        return copies

    def dn_copies(pair, s):
        copies = []
        for q in range(2):
            cols = pl.ds(pl.multiple_of(lax.rem(2 * pair + q, dn_tiles) * BLOCK, BLOCK), BLOCK)
            copies.append(pltpu.make_async_copy(wd_ref.at[:, cols], arena.at[s, pl.ds(q * hidden, hidden), :], d_sem.at[s, q]))
        return copies

    def start(copies):
        for j, c in enumerate(copies):
            c.start(priority=j % 2)

    def wait(copies):
        for c in copies:
            c.wait()

    for c in adapters[:2] + gu_copies(0, 0, False):
        c.start(priority=1)

    place, slot = route(ids_ref[...], hot_ref, group, n_local, n_hot, float(cap))
    place_i = place.astype(I32)
    slot_b = jnp.broadcast_to(slot, (128, tok)).astype(BF16)
    def sort_rows(first, arrive):
        sels = []
        for m in range(first, first + half, SUB_ROWS):
            sel = (lax.broadcasted_iota(I32, (SUB_ROWS, tok), 0) + m == place_i).astype(F32).astype(BF16)
            meta[pl.ds(m, SUB_ROWS), :] = nt_dot(sel, slot_b).astype(BF16)
            sels.append(sel)
        for n in range(0, dim, BLOCK):
            if arrive:
                for i in range(2):
                    x_copies[n // BLOCK * 2 + i].wait()
            for j, sel in enumerate(sels):
                rows = nn_dot(sel[:, :half], h_recv[:, n:n + BLOCK]) + nn_dot(sel[:, half:], h_recv[:, dim + n:dim + n + BLOCK])
                xs[pl.ds(first + j * SUB_ROWS, SUB_ROWS), n:n + BLOCK] = rows.astype(BF16)

    sort_rows(0, True)

    pl.semaphore_wait(barrier, group - 1)

    def x_copy(k):
        peer = lax.rem(me + k, group)
        src, dst = pl.ds(pl.multiple_of(peer * cap, cap), cap), pl.ds(pl.multiple_of(me * cap, cap), cap)
        return (
            pltpu.make_async_remote_copy(xs.at[src, :], recv.at[dst, :], send_sem.at[k - 1], got_sem.at[k - 1], device_id={"data": peer}, device_id_type=MESH),
            pltpu.make_async_remote_copy(meta.at[src, :], recv_meta.at[dst, :], msend_sem.at[k - 1], mgot_sem.at[k - 1], device_id={"data": peer}, device_id_type=MESH),
        )

    for k in range(1, group):
        for c in x_copy(k):
            c.start()

    for c in adapters[2:]:
        c.start(priority=1)

    sort_rows(half, False)
    place_t[...] = jnp.transpose(jnp.broadcast_to(place, (128, tok))).astype(I32)
    place_out = pltpu.make_async_copy(place_t, place_ref, out_sem.at[1])
    place_out.start()
    mine = pl.ds(pl.multiple_of(me * cap, cap), cap)
    recv[mine, :] = xs[mine, :]
    recv_meta[mine, :] = meta[mine, :]

    def keep(low, slots, width):
        cols = jnp.concatenate([slots.astype(F32)] * (width // 128), axis=1)
        lanes = lax.div(lax.broadcasted_iota(I32, cols.shape, 1), jnp.full(cols.shape, rank_dim, I32)).astype(F32)
        return jnp.where(cols == lanes, low, 0.0).astype(BF16)

    def delta(low, mat):
        return (scale * nn_dot(low, mat)).astype(BF16).astype(F32)

    def gate_up(rows_ref, rows, slots, width, h_ref, start_next):
        low_g[:, :width] = keep(nt_dot(rows_ref[rows, :], at_g[:width, :]), slots, width)
        low_u[:, :width] = keep(nt_dot(rows_ref[rows, :], at_u[:width, :]), slots, width)
        with_store = width > hot_w

        def block(tile, s, q):
            cols = pl.ds(pl.multiple_of(tile * BLOCK, BLOCK), BLOCK)
            for m in range(0, half, SUB_ROWS):
                sub, src = slice(m, m + SUB_ROWS), slice(rows.start + m, rows.start + m + SUB_ROWS)
                add_g = delta(low_g[sub, :width], arena[s, bg_row + q * both:bg_row + q * both + width, :])
                g = nn_dot(rows_ref[src, :], arena[s, g_row + q * dim:g_row + (q + 1) * dim, :]) + add_g
                add_u = delta(low_u[sub, :width], arena[s, bu_row + q * both:bu_row + q * both + width, :])
                u = nn_dot(rows_ref[src, :], arena[s, u_row + q * dim:u_row + (q + 1) * dim, :]) + add_u
                h_ref[sub, cols] = (jax.nn.silu(g) * u).astype(BF16)

        @pl.loop(0, gu_pairs)
        def _(i):
            s = lax.rem(i, 2)
            wait(gu_copies(i, s, with_store))
            start(gu_copies(i + 1, 1 - s, with_store))
            for q in range(2):
                block(2 * i + q, s, q)

        s = gu_pairs % 2
        wait(gu_copies(gu_pairs, s, with_store))
        start_next()
        block(gu_tiles - 1, s, 0)

    for c in adapters[:2]:
        c.wait()
    kept_rows = slice(half, tok)
    gate_up(xs, kept_rows, meta[kept_rows, :], hot_w, h_kept, lambda: start(gu_copies(0, 0, True)))

    for c in adapters[2:]:
        c.wait()
    for k in range(1, group):
        for c in x_copy(k):
            c.wait_recv()
    gate_up(recv, slice(0, half), recv_meta[...], both, h_recv, lambda: start(dn_copies(0, 0)))

    def back_copy(p, k):
        peer = lax.rem(me + k, group)
        cols = pl.ds(pl.multiple_of(p * (BLOCK), BLOCK), BLOCK)
        return pltpu.make_async_remote_copy(
            recv.at[pl.ds(pl.multiple_of(peer * cap, cap), cap), cols], back_ref.at[pl.ds(pl.multiple_of(me * cap, cap), cap), cols],
            bsend_sem.at[p, k - 1], bgot_sem.at[p, k - 1], device_id={"data": peer}, device_id_type=MESH)

    def down(h_ref, rows_ref, rows, slots, width, after):
        low_d[:, :width] = keep(nt_dot(h_ref[...], at_d[:width, :]), slots, width)

        @pl.loop(0, dn_tiles // 2)
        def _(i):
            s = lax.rem(i, 2)
            wait(dn_copies(i, s))
            start(dn_copies(i + 1, 1 - s))
            for q in range(2):
                p = 2 * i + q
                cols = pl.ds(pl.multiple_of(p * BLOCK, BLOCK), BLOCK)
                for m in range(0, half, SUB_ROWS):
                    sub, src = slice(m, m + SUB_ROWS), slice(rows.start + m, rows.start + m + SUB_ROWS)
                    add_y = delta(low_d[sub, :width], b_d[:width, cols])
                    y = nn_dot(h_ref[sub, :], arena[s, q * hidden:(q + 1) * hidden, :]) + add_y
                    rows_ref[src, cols] = (rows_ref[src, cols].astype(F32) + y).astype(BF16)
                after(p)

    def send_back(p):
        for k in range(1, group):
            back_copy(p, k).start()

    down(h_recv, recv, slice(0, half), recv_meta[...], both, send_back)
    own = pltpu.make_async_copy(recv.at[mine, :], back_ref.at[mine, :], out_sem.at[0])
    own.start()

    def kept_copy(p):
        cols = pl.ds(pl.multiple_of(p * BLOCK, BLOCK), BLOCK)
        return pltpu.make_async_copy(xs.at[pl.ds(half, half), cols], kept_ref.at[:, cols], kept_sem.at[p])

    down(h_kept, xs, kept_rows, meta[kept_rows, :], hot_w, lambda p: kept_copy(p).start())
    wait(dn_copies(0, 0))
    own.wait()
    place_out.wait()
    for k in range(1, group):
        for c in x_copy(k):
            c.wait_send()

    @pl.loop(0, dn_tiles)
    def _(p):
        for k in range(1, group):
            back_copy(p, k).wait()
        kept_copy(p).wait()


def unsort_kernel(place_ref, back_ref, kept_ref, out_ref, place, rows, sel, done, place_sem, sem, out_sem):
    tok, dim = out_ref.shape
    half = tok // 2
    parts = dim // BLOCK

    def load(n):
        cols = pl.ds(n * BLOCK, BLOCK)
        return [pltpu.make_async_copy(ref.at[:, cols], rows.at[pl.ds(j * half, half), cols], sem.at[n, j]) for j, ref in enumerate((back_ref, kept_ref))]

    def store(n):
        return pltpu.make_async_copy(done.at[n % 2], out_ref.at[:, pl.ds(n * BLOCK, BLOCK)], out_sem.at[n % 2])

    first = pltpu.make_async_copy(place_ref, place, place_sem.at[0])
    first.start(priority=0)
    loads = [load(n) for n in range(parts)]
    for copies in loads:
        for c in copies:
            c.start(priority=1)
    first.wait()
    for t in range(0, tok, SUB_ROWS):
        spots = jnp.concatenate([place[t:t + SUB_ROWS, :]] * (tok // 128), axis=1)
        sel[t:t + SUB_ROWS, :] = (spots == lax.broadcasted_iota(I32, (SUB_ROWS, tok), 1)).astype(F32).astype(BF16)
    for n in range(parts):
        for c in loads[n]:
            c.wait()
        if n >= 2:
            store(n - 2).wait()
        cols = slice(n * BLOCK, (n + 1) * BLOCK)
        done[n % 2] = (nn_dot(sel[:, :half], rows[:half, cols]) + nn_dot(sel[:, half:], rows[half:, cols])).astype(BF16)
        store(n).start()
    for n in range(max(parts - 2, 0), parts):
        store(n).wait()


def solution(mesh):
    group = mesh.shape["data"]
    token_spec = P(("replica", "data"), None)
    store_spec = P("data", None, None)
    full_mat = P(None, None)
    full_set = P(None, None, None)
    in_specs = (token_spec, P(("replica", "data")), full_mat, full_mat, full_mat) + (store_spec,) * 6 + (P(None),) + (full_set,) * 6

    def device_step(x, adapter_id, w_gate, w_up, w_down, a_gate, b_gate, a_up, b_up, a_down, b_down, hot_ids, hot_a_gate, hot_b_gate, hot_a_up, hot_b_up, hot_a_down, hot_b_down):
        tok, dim = x.shape
        hidden = w_gate.shape[1]
        n_local, _, rank_dim = a_gate.shape
        n_hot = hot_ids.shape[0]
        cap = tok // (2 * group)
        half = tok // 2
        both = (n_hot + n_local) * rank_dim
        cfg = (group, cap, n_local, n_hot, rank_dim, LORA_ALPHA / rank_dim)

        def rows_of(a):
            return jnp.swapaxes(a, 1, 2).reshape(-1, a.shape[1])

        def flat(b):
            return b.reshape(-1, b.shape[2])

        any_spec = pl.BlockSpec(memory_space=pl.ANY)
        vmem_spec = pl.BlockSpec(memory_space=pltpu.VMEM)
        dma = pltpu.SemaphoreType.DMA
        place, back, kept = pl.pallas_call(
            functools.partial(main_kernel, cfg),
            out_shape=(
                jax.ShapeDtypeStruct((tok, 128), I32),
                jax.ShapeDtypeStruct((half, dim), BF16),
                jax.ShapeDtypeStruct((half, dim), BF16),
            ),
            in_specs=[vmem_spec, pl.BlockSpec(memory_space=pltpu.SMEM)] + [any_spec] * 16,
            out_specs=(any_spec, any_spec, any_spec),
            scratch_shapes=[
                pltpu.VMEM((tok, dim), BF16),
                pltpu.VMEM((tok, 128), BF16),
                pltpu.VMEM((half, dim), BF16),
                pltpu.VMEM((half, 128), BF16),
                pltpu.VMEM((half, hidden), BF16),
                pltpu.VMEM((half, hidden), BF16),
                pltpu.VMEM((both, dim), BF16),
                pltpu.VMEM((both, dim), BF16),
                pltpu.VMEM((both, hidden), BF16),
                pltpu.VMEM((both, dim), BF16),
                pltpu.VMEM((2, max(4 * dim + 4 * both, 2 * hidden), BLOCK), BF16),
                pltpu.VMEM((half, both), BF16),
                pltpu.VMEM((half, both), BF16),
                pltpu.VMEM((half, both), BF16),
                pltpu.VMEM((tok, 128), I32),
                dma((dim // BLOCK, 2)), dma((2, 2, 6)), dma((2, 2)), dma((8,)), dma((2,)),
                dma((group - 1,)), dma((group - 1,)), dma((group - 1,)), dma((group - 1,)),
                dma((dim // BLOCK, group - 1)), dma((dim // BLOCK, group - 1)), dma((dim // BLOCK,)),
            ],
            compiler_params=pltpu.CompilerParams(collective_id=0, has_side_effects=True, vmem_limit_bytes=66_000_000),
            name="mlp_exchange",
        )(adapter_id.reshape(1, tok), hot_ids, x, w_gate, w_up, w_down,
          rows_of(a_gate), flat(b_gate), rows_of(a_up), flat(b_up), rows_of(a_down), flat(b_down),
          rows_of(hot_a_gate), flat(hot_b_gate), rows_of(hot_a_up), flat(hot_b_up), rows_of(hot_a_down), flat(hot_b_down))

        return pl.pallas_call(
            unsort_kernel,
            out_shape=jax.ShapeDtypeStruct((tok, dim), BF16),
            in_specs=[any_spec] * 3,
            out_specs=any_spec,
            scratch_shapes=[
                pltpu.VMEM((tok, 128), I32),
                pltpu.VMEM((tok, dim), BF16),
                pltpu.VMEM((tok, tok), BF16),
                pltpu.VMEM((2, tok, BLOCK), BF16),
                dma((1,)),
                dma((dim // BLOCK, 2)),
                dma((2,)),
            ],
            name="unsort",
        )(place, back, kept)

    return jax.shard_map(device_step, mesh=mesh, in_specs=in_specs, out_specs=token_spec, check_vma=False)
```
